32 devices in a mesh: dp: 2 (over x), tp: 4 (over z), cp: 4 (over y, core).
Axes of the slice: x: 2, y: 2, z: 4, core: 2. Of those that a mesh axis runs over, the one named last changes fastest.
Arguments:
- x: bfloat16 [16384, 4096], P(('dp', 'cp', 'tp')), parts along dimension 0
- w_q: bfloat16 [4096, 4096], P(None, 'tp')
- w_k: bfloat16 [4096, 1024], P(None, 'tp')
- w_v: bfloat16 [4096, 1024], P(None, 'tp')
- w_o: bfloat16 [4096, 4096], P('tp')
Outputs:
- output: bfloat16 [16384, 4096], P(('dp', 'cp', 'tp')), parts along dimension 0
There are 2 independent parts. The reference program is written for one: setup_inputs(seed, part) draws one part's arguments, and reference() takes and returns one part's arrays. A program takes and returns all parts, laid end to end along the dimension named above; an argument that names none is the same for every part.
All inputs are finite; a program needn't handle non-finite values.
Results may differ from the reference program's by a relative error of at most 0.0055191.
Values are sent between devices in bfloat16 or wider.
A program may use at most 1 GiB of HBM per device.

```python
import jax
import jax.numpy as jnp
from jax import lax

D = 4096
HEADS = 32
KV_HEADS = 8
HEAD = 128
SEQ = 8192
CP = 4
Q_BLOCK = 128


def stored_positions():
    piece_len = SEQ // (2 * CP)
    row_idx = jnp.arange(SEQ)
    block_idx = row_idx // (2 * piece_len)
    within = row_idx % (2 * piece_len)
    return jnp.where(within < piece_len, block_idx * piece_len + within, (2 * CP - 1 - block_idx) * piece_len + within - piece_len)


def setup_inputs(seed: int = 0, part: int = 0) -> dict:
    base_key = jax.random.key(seed)
    key_x = jax.random.fold_in(jax.random.fold_in(base_key, 1), part)
    key_q, key_k, key_v, key_o = jax.random.split(jax.random.fold_in(base_key, 2), 4)
    x_val = jax.random.normal(key_x, (SEQ, D), jnp.float32)
    w_q = jax.random.normal(key_q, (D, HEADS * HEAD), jnp.float32) * (1.6 * D ** -0.5)
    w_k = jax.random.normal(key_k, (D, KV_HEADS * HEAD), jnp.float32) * (1.6 * D ** -0.5)
    w_v = jax.random.normal(key_v, (D, KV_HEADS * HEAD), jnp.float32) * (D ** -0.5)
    w_o = jax.random.normal(key_o, (HEADS * HEAD, D), jnp.float32) * (3.0 * (HEADS * HEAD) ** -0.5)
    return {"x": x_val.astype(jnp.bfloat16), "w_q": w_q.astype(jnp.bfloat16), "w_k": w_k.astype(jnp.bfloat16), "w_v": w_v.astype(jnp.bfloat16), "w_o": w_o.astype(jnp.bfloat16)}


def reference(x, w_q, w_k, w_v, w_o):
    group_size = HEADS // KV_HEADS
    score_scale = HEAD ** -0.5
    q_proj = jnp.dot(x, w_q, preferred_element_type=jnp.float32).astype(jnp.bfloat16)
    k_proj = jnp.dot(x, w_k, preferred_element_type=jnp.float32).astype(jnp.bfloat16)
    v_proj = jnp.dot(x, w_v, preferred_element_type=jnp.float32).astype(jnp.bfloat16)
    q_blocks = q_proj.astype(jnp.float32).reshape(SEQ // Q_BLOCK, Q_BLOCK, KV_HEADS, group_size, HEAD)
    k_heads = jnp.transpose(k_proj.astype(jnp.float32).reshape(SEQ, KV_HEADS, HEAD), (1, 0, 2))
    v_heads = jnp.transpose(v_proj.astype(jnp.float32).reshape(SEQ, KV_HEADS, HEAD), (1, 0, 2))
    positions = stored_positions()
    pos_blocks = positions.reshape(SEQ // Q_BLOCK, Q_BLOCK)

    def one_block(block_args):
        q_blk, pos_blk = block_args
        visible = pos_blk[:, None] >= positions[None, :]

        def one_head(head_args):
            q_head, k_head, v_head = head_args
            scores = jnp.einsum("qge,ke->gqk", q_head, k_head) * score_scale
            scores = jnp.where(visible[None], scores, -jnp.inf)
            row_max = scores.max(axis=-1, keepdims=True)
            p_block = jnp.exp(scores - row_max)
            row_sum = p_block.sum(axis=-1)
            weighted = jnp.einsum("gqk,ke->qge", p_block.astype(jnp.bfloat16).astype(jnp.float32), v_head)
            return weighted / jnp.transpose(row_sum)[:, :, None]

        head_outs = lax.map(one_head, (jnp.transpose(q_blk, (1, 0, 2, 3)), k_heads, v_heads))
        return jnp.transpose(head_outs, (1, 0, 2, 3))

    attn_out = lax.map(one_block, (q_blocks, pos_blocks))
    attn_out = attn_out.reshape(SEQ, HEADS * HEAD).astype(jnp.bfloat16)
    return jnp.dot(attn_out, w_o, preferred_element_type=jnp.float32).astype(jnp.bfloat16)
```

```python
import functools

import jax
import jax.numpy as jnp
from jax import lax
from jax.experimental import pallas as pl
from jax.experimental.pallas import tpu as pltpu
from jax.sharding import PartitionSpec as P

D = 128
LOG2E = 1.4426950408889634


def flash_kernel(pos_ref, q_ref, k_ref, vt_ref, o_ref, m_ref, l_ref, acc_ref, *, bq, bk, group):
    c = LOG2E * D ** -0.5
    qpos = pos_ref[pl.program_id(1)]

    def tile(kstart, size, mode):
        k = k_ref[pl.ds(kstart, size), :]
        vt = vt_ref[:, pl.ds(kstart, size)]
        for g in range(group):
            q = q_ref[:, g * D:(g + 1) * D]
            s = lax.dot_general(k, q, (((1,), (1,)), ((), ())), preferred_element_type=jnp.float32)
            if mode == "diag":
                ki = lax.broadcasted_iota(jnp.int32, (size, bq), 0)
                qi = lax.broadcasted_iota(jnp.int32, (size, bq), 1)
                s = jnp.where(ki <= qi, s, -jnp.inf)
            m_cur = jnp.max(s, axis=0, keepdims=True)
            if mode == "diag":
                m_new = m_cur
            else:
                m_old = m_ref[g]
                m_new = jnp.maximum(m_old, m_cur)
            p = jnp.exp2((s - m_new) * c)
            l_cur = jnp.sum(p, axis=0, keepdims=True)
            pv = jnp.dot(vt, p.astype(jnp.bfloat16), preferred_element_type=jnp.float32)
            if mode == "diag":
                l_ref[g] = l_cur
                acc_ref[g] = pv
            else:
                alpha = jnp.exp2((m_old - m_new) * c)
                l_ref[g] = l_ref[g] * alpha + l_cur
                acc_ref[g] = acc_ref[g] * alpha + pv
            m_ref[g] = m_new

    tile(pl.multiple_of(qpos, bq), bq, "diag")
    nbig = qpos // bk

    @pl.loop(0, nbig)
    def _(i):
        tile(pl.multiple_of(i * bk, bk), bk, "full")

    @pl.loop(0, (qpos - nbig * bk) // bq)
    def _(i):
        tile(pl.multiple_of(nbig * bk + i * bq, bq), bq, "full")

    for g in range(group):
        o = acc_ref[g] / l_ref[g]
        o_ref[:, g * D:(g + 1) * D] = o.T.astype(jnp.bfloat16)


def flash(pos, q, k, vt, *, bq, bk, group):
    rows = q.shape[0]
    keys = k.shape[0]
    nkv = k.shape[1] // D
    return pl.pallas_call(
        functools.partial(flash_kernel, bq=bq, bk=bk, group=group),
        out_shape=jax.ShapeDtypeStruct((rows, nkv * group * D), jnp.bfloat16),
        grid_spec=pltpu.PrefetchScalarGridSpec(
            num_scalar_prefetch=1,
            grid=(nkv, rows // bq),
            in_specs=[
                pl.BlockSpec((bq, group * D), lambda h, i, pos: (i, h)),
                pl.BlockSpec((keys, D), lambda h, i, pos: (0, h)),
                pl.BlockSpec((D, keys), lambda h, i, pos: (h, 0)),
            ],
            out_specs=pl.BlockSpec((bq, group * D), lambda h, i, pos: (i, h)),
            scratch_shapes=[
                pltpu.VMEM((group, 1, bq), jnp.float32),
                pltpu.VMEM((group, 1, bq), jnp.float32),
                pltpu.VMEM((group, D, bq), jnp.float32),
            ],
        ),
        compiler_params=pltpu.CompilerParams(vmem_limit_bytes=56 * 1024 * 1024),
        cost_estimate=pl.CostEstimate(flops=70_000_000_000, bytes_accessed=32 * 1024 * 1024, transcendentals=67_000_000),
    )(pos, q, k, vt)


def out_kernel(o_ref, w_ref, y_ref):
    y_ref[...] = jnp.dot(o_ref[...], w_ref[0], preferred_element_type=jnp.float32).astype(jnp.bfloat16)


def out_proj(o, w):
    rows, depth = o.shape
    parts, _, cols = w.shape
    return pl.pallas_call(
        out_kernel,
        out_shape=jax.ShapeDtypeStruct((rows, parts * cols), jnp.bfloat16),
        grid=(parts,),
        in_specs=[pl.BlockSpec((rows, depth), lambda i: (0, 0)), pl.BlockSpec((1, depth, cols), lambda i: (i, 0, 0))],
        out_specs=pl.BlockSpec((rows, cols), lambda i: (0, i)),
        compiler_params=pltpu.CompilerParams(vmem_limit_bytes=48 * 1024 * 1024),
        cost_estimate=pl.CostEstimate(flops=2 * rows * depth * parts * cols, bytes_accessed=2 * depth * parts * cols, transcendentals=0),
    )(o, w)


def solution(mesh):
    cp_size = mesh.shape["cp"]
    dp_size = mesh.shape["dp"]
    row_spec = P(("dp", "cp", "tp"), None)

    def local_layer(x_loc, w_q, w_k, w_v, w_o):
        group = w_q.shape[1] // w_k.shape[1]
        parts = dp_size * cp_size
        cols = w_o.shape[1] // parts
        part = lax.axis_index("dp") * cp_size + lax.axis_index("cp")
        x_block = lax.all_gather(x_loc, "tp", axis=0, tiled=True)
        piece_len = x_block.shape[0] // 2
        k_all = jnp.dot(x_block, w_k, preferred_element_type=jnp.float32).astype(jnp.bfloat16)
        vt_all = lax.dot_general(w_v, x_block, (((0,), (1,)), ((), ())), preferred_element_type=jnp.float32).astype(jnp.bfloat16)
        k_g = lax.all_gather(k_all, "cp", axis=0).reshape(cp_size, 2, piece_len, -1)
        vt_g = lax.all_gather(vt_all, "cp", axis=0).reshape(cp_size, -1, 2, piece_len)
        q_all = jnp.dot(x_block, w_q, preferred_element_type=jnp.float32).astype(jnp.bfloat16)
        w_part = lax.dynamic_slice_in_dim(w_o, part * cols, cols, axis=1)
        w_part = lax.all_gather(w_part, "tp", axis=0, tiled=True)
        w_full = lax.all_gather(w_part, ("dp", "cp"), axis=0)
        k_pos = jnp.concatenate([k_g[:, 0], k_g[::-1, 1]]).reshape(2 * cp_size * piece_len, -1)
        vt_pos = jnp.concatenate([vt_g[:, :, 0], vt_g[::-1, :, 1]]).transpose(1, 0, 2).reshape(-1, 2 * cp_size * piece_len)
        bq = 512
        rank = lax.axis_index("cp")
        steps = jnp.arange(piece_len // bq, dtype=jnp.int32) * bq
        pos = jnp.concatenate([rank * piece_len + steps, (2 * cp_size - 1 - rank) * piece_len + steps]).astype(jnp.int32)
        o = flash(pos, q_all, k_pos, vt_pos, bq=bq, bk=1024, group=group)
        o_rows = lax.all_to_all(o, "tp", split_axis=0, concat_axis=1, tiled=True)
        return out_proj(o_rows, w_full)

    return jax.shard_map(local_layer, mesh=mesh, in_specs=(row_spec, P(None, "tp"), P(None, "tp"), P(None, "tp"), P("tp", None)), out_specs=row_spec, check_vma=False)
```

```python
import functools

import jax
import jax.numpy as jnp
from jax import lax
from jax.experimental import pallas as pl
from jax.experimental.pallas import tpu as pltpu
from jax.sharding import PartitionSpec as P


D = 128
T = 512
WIDTH = 2
LOG2E = 1.4426950408889634


def flash_kernel(q_ref, *refs, group, cp_size, nkv, head):
    tiles = 4 * cp_size
    kv_in, (o_ref, kv_ref, m_ref, l_ref, acc_ref, s_ref, sems) = refs[:tiles], refs[tiles:]
    c = LOG2E * D ** -0.5
    z = lax.axis_index("tp")
    r = lax.axis_index("cp")
    h = pl.program_id(0)

    def flip(v, bit):
        return v + bit - 2 * bit * ((v // bit) % 2)

    def seq_tile(far, core, row, near):
        src_z, src_r = z, r
        for on, bit in ((far, 2), (near, 1)):
            src_z = flip(src_z, bit) if on else src_z
        for on, bit in ((row, 2), (core, 1)):
            src_r = flip(src_r, bit) if on else src_r
        piece = jnp.where(src_z < 2, src_r, 2 * cp_size - 1 - src_r)
        return 2 * piece + src_z % 2

    slot = pl.program_id(1)
    qt = jnp.where(slot == 0, seq_tile(1, 0, 0, 0), seq_tile(0, 0, 0, 0))

    @pl.when((h == 0) & (slot == 0))
    def _():
        copies = []
        for j in range(tiles):
            pos = seq_tile(j // 8, j // 4 % 2, j // 2 % 2, j % 2)
            copies.append(pltpu.make_async_copy(kv_in[j], kv_ref.at[pos], sems.at[j]))
        for copy in copies:
            copy.start()
        for copy in copies:
            copy.wait()

    k_cols = pl.ds(pl.multiple_of((head + h) * D, D), D)
    v_cols = pl.ds(pl.multiple_of((nkv + head + h) * D, D), D)

    def step(ts, diag):
        ks = [kv_ref[t, :, k_cols] for t in ts]
        vs = [kv_ref[t, :, v_cols] for t in ts]

        def front(g):
            q = q_ref[:, g * D:(g + 1) * D]
            ss = [lax.dot_general(k, q, (((1,), (1,)), ((), ())), preferred_element_type=jnp.float32) for k in ks]
            if diag:
                ki = lax.broadcasted_iota(jnp.int32, (T, T), 0)
                qi = lax.broadcasted_iota(jnp.int32, (T, T), 1)
                ss = [jnp.where(ki <= qi, ss[0], -jnp.inf)]
            for j, s in enumerate(ss):
                s_ref[g % 2, j] = s
            return functools.reduce(jnp.maximum, [jnp.max(s, axis=0, keepdims=True) for s in ss])

        def back(g, m_new):
            if not diag:
                m_old = m_ref[g]
                m_new = jnp.maximum(m_old, m_new)
            ps = [jnp.exp2((s_ref[g % 2, j] - m_new) * c) for j in range(len(ts))]
            l_cur = functools.reduce(jnp.add, [jnp.sum(p, axis=0, keepdims=True) for p in ps])
            pv = functools.reduce(jnp.add, [
                lax.dot_general(v, p.astype(jnp.bfloat16), (((0,), (0,)), ((), ())), preferred_element_type=jnp.float32)
                for v, p in zip(vs, ps)])
            if diag:
                l_ref[g] = l_cur
                acc_ref[g] = pv
            else:
                alpha = jnp.exp2((m_old - m_new) * c)
                l_ref[g] = l_ref[g] * alpha + l_cur
                acc_ref[g] = acc_ref[g] * alpha + pv
            m_ref[g] = m_new

        m_cur = front(0)
        for g in range(group):
            m_nxt = front(g + 1) if g + 1 < group else None
            back(g, m_cur)
            m_cur = m_nxt

    step([qt], True)

    @pl.loop(0, qt // WIDTH)
    def _(i):
        step([WIDTH * i + j for j in range(WIDTH)], False)

    @pl.loop(qt // WIDTH * WIDTH, qt)
    def _(i):
        step([i], False)

    for g in range(group):
        o = acc_ref[g] / l_ref[g]
        o_ref[:, g * D:(g + 1) * D] = o.T.astype(jnp.bfloat16)


def flash(q, tiles, *, group, cp_size, heads=None):
    nkv = tiles[0].shape[1] // (2 * D)
    heads = heads or tuple(range(nkv))
    return pl.pallas_call(
        functools.partial(flash_kernel, group=group, cp_size=cp_size, nkv=nkv, head=heads[0]),
        out_shape=jax.ShapeDtypeStruct((2 * T, len(heads) * group * D), jnp.bfloat16),
        grid=(len(heads), 2),
        in_specs=[pl.BlockSpec((T, group * D), lambda h, i: (i, heads[0] + h))] + [pl.BlockSpec(memory_space=pltpu.HBM)] * len(tiles),
        out_specs=pl.BlockSpec((T, group * D), lambda h, i: (i, h)),
        scratch_shapes=[
            pltpu.VMEM((len(tiles), T, 2 * nkv * D), jnp.bfloat16),
            pltpu.VMEM((group, 1, T), jnp.float32),
            pltpu.VMEM((group, 1, T), jnp.float32),
            pltpu.VMEM((group, D, T), jnp.float32),
            pltpu.VMEM((2, WIDTH, T, T), jnp.float32),
            pltpu.SemaphoreType.DMA((len(tiles),)),
        ],
        compiler_params=pltpu.CompilerParams(vmem_limit_bytes=66_000_000),
        cost_estimate=pl.CostEstimate(flops=20_000_000_000, bytes_accessed=12 * 1024 * 1024, transcendentals=17_000_000),
    )(q, *tiles)


def out_kernel(*refs, counts):
    refs, y_ref = list(refs[:-1]), refs[-1]
    o_groups = [[refs.pop(0) for _ in range(n)] for n in counts]
    acc = None
    for os, w in zip(o_groups, refs):
        start = 0
        for o in os:
            rows = slice(start, start + o.shape[1])
            w_rows = w[rows] if len(w.shape) == 2 else w[0, rows]
            term = jnp.dot(o[...], w_rows, preferred_element_type=jnp.float32)
            acc = term if acc is None else acc + term
            start += o.shape[1]
    y_ref[...] = acc.astype(jnp.bfloat16)


def out_proj(o_groups, ws):
    os = [o for group, _ in o_groups for o in group]
    places = [place for group, place in o_groups for _ in group]
    rows = T
    parts, depth, cols = ws[1].shape
    w_spec = pl.BlockSpec((1, depth, cols), lambda i: (i, 0, 0))
    return pl.pallas_call(
        functools.partial(out_kernel, counts=[len(group) for group, _ in o_groups]),
        out_shape=jax.ShapeDtypeStruct((rows, parts * cols), jnp.bfloat16),
        grid=(parts,),
        in_specs=[pl.BlockSpec((rows, o.shape[1]), lambda i, place=place: (place, 0)) for o, place in zip(os, places)] + [pl.BlockSpec((depth, cols), lambda i: (0, i))] + [w_spec] * 3,
        out_specs=pl.BlockSpec((rows, cols), lambda i: (0, i)),
        compiler_params=pltpu.CompilerParams(vmem_limit_bytes=66_000_000),
        cost_estimate=pl.CostEstimate(flops=8 * rows * depth * parts * cols, bytes_accessed=8 * depth * parts * cols, transcendentals=0),
    )(*os, *ws)


def swap(x, axis, size, bit):
    return lax.ppermute(x, axis, [(i, i ^ bit) for i in range(size)])


def project(x, w):
    return jnp.dot(x, w, preferred_element_type=jnp.float32).astype(jnp.bfloat16)


def after(x, *others):
    return lax.optimization_barrier((x, *others))[0]


def solution(mesh):
    cp_size = mesh.shape["cp"]
    dp_size = mesh.shape["dp"]
    tp_size = mesh.shape["tp"]
    row_spec = P(("dp", "cp", "tp"), None)

    def local_layer(x_own, w_q, w_k, w_v, w_o):
        group = w_q.shape[1] // w_k.shape[1]
        parts = dp_size * cp_size
        part = lax.axis_index("dp") * cp_size + lax.axis_index("cp")

        def own_part(w, axis):
            size = w.shape[axis] // parts
            return lax.dynamic_slice_in_dim(w, part * size, size, axis=axis)

        def tp(x, bit):
            return swap(x, "tp", tp_size, bit)

        def cp(x, bit):
            return swap(x, "cp", cp_size, bit)

        def hops(kv, kv_near):
            first = [kv, kv_near]
            four = first + [cp(t, 2) for t in first]
            return four + [cp(t, 1) for t in four]

        def direct(kv, kv_near):
            tiles = []
            for bits in (0, 2, 1, 3):
                for t in (kv, kv_near):
                    tiles.append(cp(t, bits) if bits else t)
            return tiles

        w_kv = jnp.concatenate([w_k, w_v], axis=1)
        kv_part = tp(jnp.concatenate([own_part(w_k, 0), own_part(w_v, 0)], axis=1), 1)
        q_part = tp(own_part(w_q, 0), 1)
        half = x_own.shape[0] // 2
        x_one = tp(x_own[:half], 2)
        kv_a_own = project(x_own, w_kv)
        w_kv_par = lax.all_gather(after(kv_part, kv_a_own), ("dp", "cp"), axis=0, tiled=True)
        w_q_par = lax.all_gather(after(q_part, kv_a_own), ("dp", "cp"), axis=0, tiled=True)
        a_near = tp(kv_a_own, 1)
        kv_b_own = project(x_own, w_kv_par)
        b_near = tp(kv_b_own, 1)
        q_a_own = project(x_own, w_q)
        q_b_own = project(x_own, w_q_par)

        o_part = own_part(w_o, 1)
        o_near = tp(o_part, 1)

        x_two = tp(after(x_own[half:], x_one, kv_b_own), 2)
        one = [project(x_one, w) for w in (w_kv, w_kv_par, w_q, w_q_par)]
        tiles_a = hops(after(kv_a_own, one[0]), after(b_near, one[0]))
        tiles_b = hops(after(kv_b_own, one[0]), after(a_near, one[0]))
        w_near = lax.all_gather(after(o_near, w_q_par, *tiles_a, *tiles_b), ("dp", "cp"), axis=0)
        x_two = after(x_two, q_a_own, q_b_own, *one, *tiles_a, *tiles_b)

        def far(i, w, own=()):
            return jnp.concatenate([one[i], project(x_two, w), *own])

        kv_a_far = far(0, w_kv)
        kv_b_far = far(1, w_kv_par)
        a_far_near = tp(kv_b_far, 1)
        far_a = hops(kv_a_far, a_far_near)
        b_far_near = tp(kv_a_far, 1)
        far_b = direct(kv_b_far, after(b_far_near, far_a[3]))
        x_two = after(x_two, kv_a_far, kv_b_far)
        q_a = far(2, w_q, [q_a_own])
        q_b = far(3, w_q_par, [q_b_own])
        tiles_a += far_a
        tiles_b += far_b
        o_far = after(tp(after(o_part, a_far_near), 2), *far_a, b_far_near)
        o_cross = tp(o_far, 1)
        w_far = lax.all_gather(o_far, ("dp", "cp"), axis=0)

        def attend(q, prior, tiles, **kw):
            return flash(after(q, *prior), tiles, group=group, cp_size=cp_size, **kw)

        out_a = attend(q_a, [q_b, o_far], tiles_a)
        got_a = tp(out_a[:T], 2)
        w_cross = lax.all_gather(after(o_cross, out_a), ("dp", "cp"), axis=0)
        tiles_b = tiles_b[:8] + [after(t, out_a) for t in tiles_b[8:]]
        out_b, got_b = [out_a], []
        for head in range(w_k.shape[1] // D):
            out_b.append(attend(q_b, out_b[-1:], tiles_b, heads=(head,)))
            got_b.append(tp(out_b[-1][:T], 2))
        return out_proj([([out_a], 1), (out_b[1:], 1), ([got_a], 0), (got_b, 0)], [w_o, w_near, w_far, w_cross])

    return jax.shard_map(local_layer, mesh=mesh, in_specs=(row_spec, P(None, "tp"), P(None, "tp"), P(None, "tp"), P("tp", None)), out_specs=row_spec, check_vma=False)
```

```python
import functools

import jax
import jax.numpy as jnp
from jax import lax
from jax.experimental import pallas as pl
from jax.experimental.pallas import tpu as pltpu
from jax.sharding import PartitionSpec as P


D = 128
T = 512
WIDTH = 2
LOG2E = 1.4426950408889634


def flash_kernel(q_ref, *refs, group, cp_size, nkv, head):
    tiles = 4 * cp_size
    kv_in, (o_ref, kv_ref, m_ref, l_ref, acc_ref, s_ref, sems) = refs[:tiles], refs[tiles:]
    c = LOG2E * D ** -0.5
    z = lax.axis_index("tp")
    r = lax.axis_index("cp")
    h = pl.program_id(0)

    def flip(v, bit):
        return v + bit - 2 * bit * ((v // bit) % 2)

    def seq_tile(far, core, row, near):
        src_z, src_r = z, r
        for on, bit in ((far, 2), (near, 1)):
            src_z = flip(src_z, bit) if on else src_z
        for on, bit in ((row, 2), (core, 1)):
            src_r = flip(src_r, bit) if on else src_r
        piece = jnp.where(src_z < 2, src_r, 2 * cp_size - 1 - src_r)
        return 2 * piece + src_z % 2

    slot = pl.program_id(1)
    qt = jnp.where(slot == 0, seq_tile(1, 0, 0, 0), seq_tile(0, 0, 0, 0))

    @pl.when((h == 0) & (slot == 0))
    def _():
        copies = []
        for j in range(tiles):
            pos = seq_tile(j // 8, j // 4 % 2, j // 2 % 2, j % 2)
            copies.append(pltpu.make_async_copy(kv_in[j], kv_ref.at[pos], sems.at[j]))
        for copy in copies:
            copy.start()
        for copy in copies:
            copy.wait()

    k_cols = pl.ds(pl.multiple_of((head + h) * D, D), D)
    v_cols = pl.ds(pl.multiple_of((nkv + head + h) * D, D), D)

    def step(ts, diag):
        ks = [kv_ref[t, :, k_cols] for t in ts]
        vs = [kv_ref[t, :, v_cols] for t in ts]

        def front(g):
            q = q_ref[:, g * D:(g + 1) * D]
            ss = [lax.dot_general(k, q, (((1,), (1,)), ((), ())), preferred_element_type=jnp.float32) for k in ks]
            if diag:
                ki = lax.broadcasted_iota(jnp.int32, (T, T), 0)
                qi = lax.broadcasted_iota(jnp.int32, (T, T), 1)
                ss = [jnp.where(ki <= qi, ss[0], -jnp.inf)]
            for j, s in enumerate(ss):
                s_ref[g % 2, j] = s
            return functools.reduce(jnp.maximum, [jnp.max(s, axis=0, keepdims=True) for s in ss])

        def back(g, m_new):
            if not diag:
                m_old = m_ref[g]
                m_new = jnp.maximum(m_old, m_new)
            ps = [jnp.exp2((s_ref[g % 2, j] - m_new) * c) for j in range(len(ts))]
            l_cur = functools.reduce(jnp.add, [jnp.sum(p, axis=0, keepdims=True) for p in ps])
            pv = functools.reduce(jnp.add, [
                lax.dot_general(v, p.astype(jnp.bfloat16), (((0,), (0,)), ((), ())), preferred_element_type=jnp.float32)
                for v, p in zip(vs, ps)])
            if diag:
                l_ref[g] = l_cur
                acc_ref[g] = pv
            else:
                alpha = jnp.exp2((m_old - m_new) * c)
                l_ref[g] = l_ref[g] * alpha + l_cur
                acc_ref[g] = acc_ref[g] * alpha + pv
            m_ref[g] = m_new

        m_cur = front(0)
        for g in range(group):
            m_nxt = front(g + 1) if g + 1 < group else None
            back(g, m_cur)
            m_cur = m_nxt

    step([qt], True)

    @pl.loop(0, qt // WIDTH)
    def _(i):
        step([WIDTH * i + j for j in range(WIDTH)], False)

    @pl.loop(qt // WIDTH * WIDTH, qt)
    def _(i):
        step([i], False)

    for g in range(group):
        o = acc_ref[g] / l_ref[g]
        o_ref[:, g * D:(g + 1) * D] = o.T.astype(jnp.bfloat16)


def flash(q, tiles, *, group, cp_size, heads=None):
    nkv = tiles[0].shape[1] // (2 * D)
    heads = heads or tuple(range(nkv))
    return pl.pallas_call(
        functools.partial(flash_kernel, group=group, cp_size=cp_size, nkv=nkv, head=heads[0]),
        out_shape=jax.ShapeDtypeStruct((2 * T, len(heads) * group * D), jnp.bfloat16),
        grid=(len(heads), 2),
        in_specs=[pl.BlockSpec((T, group * D), lambda h, i: (i, heads[0] + h))] + [pl.BlockSpec(memory_space=pltpu.HBM)] * len(tiles),
        out_specs=pl.BlockSpec((T, group * D), lambda h, i: (i, h)),
        scratch_shapes=[
            pltpu.VMEM((len(tiles), T, 2 * nkv * D), jnp.bfloat16),
            pltpu.VMEM((group, 1, T), jnp.float32),
            pltpu.VMEM((group, 1, T), jnp.float32),
            pltpu.VMEM((group, D, T), jnp.float32),
            pltpu.VMEM((2, WIDTH, T, T), jnp.float32),
            pltpu.SemaphoreType.DMA((len(tiles),)),
        ],
        compiler_params=pltpu.CompilerParams(vmem_limit_bytes=66_000_000),
        cost_estimate=pl.CostEstimate(flops=20_000_000_000, bytes_accessed=12 * 1024 * 1024, transcendentals=17_000_000),
    )(q, *tiles)


def out_kernel(*refs, counts):
    refs, y_ref = list(refs[:-1]), refs[-1]
    o_groups = [[refs.pop(0) for _ in range(n)] for n in counts]
    acc = refs.pop()[...] if len(refs) > len(counts) else None
    for os, w in zip(o_groups, refs):
        start = 0
        for o in os:
            rows = slice(start, start + o.shape[1])
            w_rows = w[rows] if len(w.shape) == 2 else w[0, rows]
            term = jnp.dot(o[...], w_rows, preferred_element_type=jnp.float32)
            acc = term if acc is None else acc + term
            start += o.shape[1]
    y_ref[...] = acc.astype(y_ref.dtype)


def out_proj(o_groups, ws, dtype, part=None):
    os = [o for group, _ in o_groups for o in group]
    places = [place for group, place in o_groups for _ in group]
    rows = T
    parts, depth, cols = ws[-1].shape
    own_spec = pl.BlockSpec((depth, cols), lambda i: (0, i))
    y_spec = pl.BlockSpec((rows, cols), lambda i: (0, i))
    return pl.pallas_call(
        functools.partial(out_kernel, counts=[len(group) for group, _ in o_groups]),
        out_shape=jax.ShapeDtypeStruct((rows, parts * cols), dtype),
        grid=(parts,),
        in_specs=[pl.BlockSpec((rows, o.shape[1]), lambda i, place=place: (place, 0)) for o, place in zip(os, places)]
        + [own_spec if w.ndim == 2 else pl.BlockSpec((1, depth, cols), lambda i: (i, 0, 0)) for w in ws]
        + [y_spec] * (part is not None),
        out_specs=y_spec,
        compiler_params=pltpu.CompilerParams(vmem_limit_bytes=66_000_000),
        cost_estimate=pl.CostEstimate(flops=2 * len(ws) * rows * depth * parts * cols, bytes_accessed=2 * len(ws) * depth * parts * cols, transcendentals=0),
    )(*os, *ws, *([] if part is None else [part]))


def swap(x, axis, size, bit):
    return lax.ppermute(x, axis, [(i, i ^ bit) for i in range(size)])


def project(x, w):
    return jnp.dot(x, w, preferred_element_type=jnp.float32).astype(jnp.bfloat16)


def after(x, *others):
    return lax.optimization_barrier((x, *others))[0]


def solution(mesh):
    cp_size = mesh.shape["cp"]
    dp_size = mesh.shape["dp"]
    tp_size = mesh.shape["tp"]
    row_spec = P(("dp", "cp", "tp"), None)

    def local_layer(x_own, w_q, w_k, w_v, w_o):
        group = w_q.shape[1] // w_k.shape[1]
        parts = dp_size * cp_size
        part = lax.axis_index("dp") * cp_size + lax.axis_index("cp")

        def own_part(w, axis):
            size = w.shape[axis] // parts
            return lax.dynamic_slice_in_dim(w, part * size, size, axis=axis)

        def tp(x, bit):
            return swap(x, "tp", tp_size, bit)

        def cp(x, bit):
            return swap(x, "cp", cp_size, bit)

        def hops(kv, kv_near):
            first = [kv, kv_near]
            four = first + [cp(t, 2) for t in first]
            return four + [cp(t, 1) for t in four]

        w_kv = jnp.concatenate([w_k, w_v], axis=1)
        kv_part = tp(jnp.concatenate([own_part(w_k, 0), own_part(w_v, 0)], axis=1), 1)
        q_part = tp(own_part(w_q, 0), 1)
        half = x_own.shape[0] // 2
        x_one = tp(x_own[:half], 2)
        kv_a_own = project(x_own, w_kv)
        w_kv_par = lax.all_gather(after(kv_part, kv_a_own), ("dp", "cp"), axis=0, tiled=True)
        w_q_par = lax.all_gather(after(q_part, kv_a_own), ("dp", "cp"), axis=0, tiled=True)
        a_near = tp(kv_a_own, 1)
        kv_b_own = project(x_own, w_kv_par)
        b_near = tp(kv_b_own, 1)
        q_a_own = project(x_own, w_q)
        q_b_own = project(x_own, w_q_par)

        o_part = own_part(w_o, 1)
        o_near = tp(o_part, 1)

        x_two = tp(after(x_own[half:], x_one, kv_b_own), 2)
        one = [project(x_one, w) for w in (w_kv, w_kv_par, w_q, w_q_par)]
        tiles_a = hops(after(kv_a_own, one[0]), after(b_near, one[0]))
        tiles_b = hops(after(kv_b_own, one[0]), after(a_near, one[0]))
        w_near = lax.all_gather(after(o_near, w_q_par, *tiles_a, *tiles_b), ("dp", "cp"), axis=0)
        x_two = after(x_two, q_a_own, q_b_own, *one, *tiles_a, *tiles_b)

        def far(i, w, own=()):
            return jnp.concatenate([one[i], project(x_two, w), *own])

        kv_a_far = far(0, w_kv)
        kv_b_far = far(1, w_kv_par)
        a_far_near = tp(kv_b_far, 1)
        far_a = hops(kv_a_far, a_far_near)
        b_far_near = tp(kv_a_far, 1)
        far_b = hops(kv_b_far, b_far_near)
        x_two = after(x_two, kv_a_far, kv_b_far)
        q_a = far(2, w_q, [q_a_own])
        q_b = far(3, w_q_par, [q_b_own])
        tiles_a += far_a
        tiles_b += far_b
        o_far = after(tp(after(o_part, a_far_near), 2), *far_a, *far_b)
        o_cross = tp(o_far, 1)
        w_far = lax.all_gather(o_far, ("dp", "cp"), axis=0)

        def attend(q, prior, tiles, **kw):
            return flash(after(q, *prior), tiles, group=group, cp_size=cp_size, **kw)

        out_a = attend(q_a, [q_b, o_far], tiles_a)
        got_a = tp(out_a[:T], 2)
        w_cross = lax.all_gather(after(o_cross, out_a), ("dp", "cp"), axis=0)
        out_b, got_b = [out_a], []
        for head in range(w_k.shape[1] // D):
            out_b.append(attend(q_b, out_b[-1:], tiles_b, heads=(head,)))
            got_b.append(tp(out_b[-1][:T], 2))
        y_part = out_proj([([out_a], 1), (out_b[1:], 1), ([got_a], 0)], [w_o, w_near, w_far], jnp.float32)
        return out_proj([(got_b, 0)], [w_cross], jnp.bfloat16, part=y_part)

    return jax.shard_map(local_layer, mesh=mesh, in_specs=(row_spec, P(None, "tp"), P(None, "tp"), P(None, "tp"), P("tp", None)), out_specs=row_spec, check_vma=False)
```
